8 devices in a mesh: batch: 2 (over z, y), seq: 4 (over x, core).
Axes of the slice: x: 2, y: 2, z: 1, core: 2. Of those that a mesh axis runs over, the one named last changes fastest.
Arguments:
- msa_act: bfloat16 [64, 384, 256], P(('batch', 'seq')), parts along dimension 0
- msa_mask: int32 [64, 384], P(('batch', 'seq')), parts along dimension 0
- pair_act: bfloat16 [768, 384, 128], P(('batch', 'seq')), parts along dimension 0
- w_pair_bias: bfloat16 [128, 8], replicated
- w_row_in: bfloat16 [256, 1024], replicated
- w_row_out: bfloat16 [256, 256], replicated
- w_col_in: bfloat16 [256, 576], replicated
- w_col_out: bfloat16 [256, 256], replicated
- w_trans_in: bfloat16 [256, 1024], replicated
- w_trans_out: bfloat16 [1024, 256], replicated
Outputs:
- output: bfloat16 [64, 384, 256], P('batch', 'seq'), parts along dimension 0
There are 2 independent parts. The reference program is written for one: setup_inputs(seed, part) draws one part's arguments, and reference() takes and returns one part's arrays. A program takes and returns all parts, laid end to end along the dimension named above; an argument that names none is the same for every part.
All inputs are finite; a program needn't handle non-finite values.
Results may differ from the reference program's by a relative error of at most 0.0153404.
Values are sent between devices in bfloat16 or wider.
A program may use at most 1 GiB of HBM per device.

```python
import jax
import jax.numpy as jnp
from jax import lax

SEQ_DEV = 8
GROUP_SIZE = 4
NUM_SEQ = 32
RESIDUES = 384
MSA_CH = 256
PAIR_CH = 128
NUM_HEADS = 8
HEAD_DIM = 32

HEAD_CH = NUM_HEADS * HEAD_DIM
COL_CH = 2 * HEAD_CH + 2 * HEAD_DIM
TRANS_CH = 4 * MSA_CH
TILE_BUDGET = 2 ** 22
LN_EPS = 1.0e-5
MASK_BIG = 1.0e9
MEAN_EPS = 1.0e-10


def draw_weight(base_key, fan_in, fan_out, gain):
    normal = jax.random.normal(base_key, (fan_in, fan_out), jnp.float32)
    return (gain * fan_in ** -0.5 * normal).astype(jnp.bfloat16)


def draw_mask(mask_key):
    key_cls, key_start, key_len = jax.random.split(mask_key, 3)
    shard_class = jax.random.randint(key_cls, (GROUP_SIZE,), 1, 5)
    len_cap = jnp.repeat(shard_class * (RESIDUES // 4), SEQ_DEV)
    starts = jax.random.randint(key_start, (NUM_SEQ,), 0, RESIDUES)
    lengths = jax.random.randint(key_len, (NUM_SEQ,), 1, len_cap + 1)
    lengths = jnp.where(jnp.arange(NUM_SEQ) == 0, RESIDUES, lengths)
    offset = (jnp.arange(RESIDUES)[None, :] - starts[:, None]) % RESIDUES
    return (offset < lengths[:, None]).astype(jnp.int32)


def setup_inputs(seed: int = 0, part: int = 0) -> dict:
    part_key = jax.random.fold_in(jax.random.key(seed), part)
    key_mask, key_shared, key_shard, key_noise, key_pair = jax.random.split(part_key, 5)
    weight_keys = jax.random.split(jax.random.key(seed + 1), 7)
    shared = jax.random.normal(key_shared, (1, RESIDUES, MSA_CH), jnp.float32)
    per_shard = jnp.repeat(jax.random.normal(key_shard, (GROUP_SIZE, RESIDUES, MSA_CH), jnp.float32), SEQ_DEV, axis=0)
    noise_part = jax.random.normal(key_noise, (NUM_SEQ, RESIDUES, MSA_CH), jnp.float32)
    msa_act = (0.7 * shared + 0.7 * per_shard + 0.7 * noise_part).astype(jnp.bfloat16)
    pair_act = jax.random.normal(key_pair, (RESIDUES, RESIDUES, PAIR_CH), jnp.float32).astype(jnp.bfloat16)
    return {
        'msa_act': msa_act,
        'msa_mask': draw_mask(key_mask),
        'pair_act': pair_act,
        'w_pair_bias': draw_weight(weight_keys[0], PAIR_CH, NUM_HEADS, 1.5),
        'w_row_in': draw_weight(weight_keys[1], MSA_CH, 4 * HEAD_CH, 1.0),
        'w_row_out': draw_weight(weight_keys[2], HEAD_CH, MSA_CH, 3.0),
        'w_col_in': draw_weight(weight_keys[3], MSA_CH, COL_CH, 1.5),
        'w_col_out': draw_weight(weight_keys[4], HEAD_CH, MSA_CH, 2.0),
        'w_trans_in': draw_weight(weight_keys[5], MSA_CH, TRANS_CH, 1.4),
        'w_trans_out': draw_weight(weight_keys[6], TRANS_CH, MSA_CH, 1.5),
    }


def layer_norm(x_in):
    x_f32 = x_in.astype(jnp.float32)
    mean_val = jnp.mean(x_f32, axis=-1, keepdims=True)
    centered = x_f32 - mean_val
    var_val = jnp.mean(centered * centered, axis=-1, keepdims=True)
    return (centered * lax.rsqrt(var_val + LN_EPS)).astype(jnp.bfloat16)


def linear(x_in, weight):
    flat_out = jnp.dot(x_in.reshape(-1, x_in.shape[-1]), weight, preferred_element_type=jnp.float32)
    return flat_out.reshape(x_in.shape[:-1] + (weight.shape[-1],))


def pick_tile(n_rows, per_row):
    best_tile = 1
    for candidate in range(1, n_rows + 1):
        if n_rows % candidate == 0 and candidate * per_row <= TILE_BUDGET:
            best_tile = candidate
    return best_tile


def to_tiles(big_array, tile_rows):
    return big_array.reshape((big_array.shape[0] // tile_rows, tile_rows) + big_array.shape[1:])


def row_tile(act_tile, mask_tile, bias_hij, w_row_in, w_row_out):
    n_rows = act_tile.shape[0]
    projected = linear(layer_norm(act_tile), w_row_in).astype(jnp.bfloat16).astype(jnp.float32)
    projected = projected.reshape(n_rows, RESIDUES, 4, NUM_HEADS, HEAD_DIM)
    logits = jnp.einsum('sihd,sjhd->shij', projected[:, :, 0], projected[:, :, 1]) * HEAD_DIM ** -0.5
    logits = logits + bias_hij[None] + mask_tile[:, None, None, :]
    attn_probs = jax.nn.softmax(logits, axis=-1).astype(jnp.bfloat16).astype(jnp.float32)
    attended = jnp.einsum('shij,sjhd->sihd', attn_probs, projected[:, :, 2])
    gated_out = (jax.nn.sigmoid(projected[:, :, 3]) * attended).astype(jnp.bfloat16)
    row_update = linear(gated_out.reshape(n_rows, RESIDUES, HEAD_CH), w_row_out)
    return (act_tile.astype(jnp.float32) + row_update).astype(jnp.bfloat16)


def col_project(act_tile, w_col_in):
    n_rows = act_tile.shape[0]
    projected = linear(layer_norm(act_tile), w_col_in).astype(jnp.bfloat16).astype(jnp.float32)
    queries = projected[:, :, :HEAD_CH].reshape(n_rows, RESIDUES, NUM_HEADS, HEAD_DIM)
    col_keys = projected[:, :, HEAD_CH:HEAD_CH + HEAD_DIM]
    col_vals = projected[:, :, HEAD_CH + HEAD_DIM:HEAD_CH + 2 * HEAD_DIM]
    col_gates = projected[:, :, HEAD_CH + 2 * HEAD_DIM:].reshape(n_rows, RESIDUES, NUM_HEADS, HEAD_DIM)
    return queries, col_keys, col_vals, col_gates


def reference(msa_act, msa_mask, pair_act, w_pair_bias, w_row_in, w_row_out, w_col_in, w_col_out, w_trans_in, w_trans_out):
    mask_f32 = msa_mask.astype(jnp.float32)
    mask_bias = MASK_BIG * (mask_f32 - 1.0)
    pair_bias = linear(layer_norm(pair_act), w_pair_bias).astype(jnp.bfloat16)
    bias_hij = jnp.transpose(pair_bias, (2, 0, 1)).astype(jnp.float32)
    tile_rows = pick_tile(NUM_SEQ, NUM_HEADS * RESIDUES * RESIDUES)

    def row_body(packed):
        return row_tile(packed[0], packed[1], bias_hij, w_row_in, w_row_out)

    after_row = lax.map(row_body, (to_tiles(msa_act, tile_rows), to_tiles(mask_bias, tile_rows)))

    def stats_body(packed):
        projected = col_project(packed[0], w_col_in)
        q_part = jnp.einsum('sn,snhd->nhd', packed[1], projected[0])
        return q_part, projected[1], projected[2]

    q_parts, col_keys, col_vals = lax.map(stats_body, (after_row, to_tiles(mask_f32, tile_rows)))
    mask_count = jnp.sum(mask_f32, axis=0)
    q_mean = (jnp.sum(q_parts, axis=0) / (mask_count + MEAN_EPS)[:, None, None]).astype(jnp.bfloat16).astype(jnp.float32)
    col_logits = jnp.einsum('nhd,snd->snh', q_mean, col_keys.reshape(NUM_SEQ, RESIDUES, HEAD_DIM)) * HEAD_DIM ** -0.5
    col_logits = col_logits + mask_bias[:, :, None]
    col_probs = jax.nn.softmax(col_logits, axis=0)
    col_out = jnp.einsum('snh,snd->nhd', col_probs, col_vals.reshape(NUM_SEQ, RESIDUES, HEAD_DIM))

    def final_body(act_tile):
        projected = col_project(act_tile, w_col_in)
        gated_out = (jax.nn.sigmoid(projected[3]) * col_out[None]).astype(jnp.bfloat16)
        col_update = linear(gated_out.reshape(act_tile.shape[0], RESIDUES, HEAD_CH), w_col_out)
        after_col = (act_tile.astype(jnp.float32) + col_update).astype(jnp.bfloat16)
        hidden = jnp.maximum(linear(layer_norm(after_col), w_trans_in), 0.0).astype(jnp.bfloat16)
        return (after_col.astype(jnp.float32) + linear(hidden, w_trans_out)).astype(jnp.bfloat16)

    return lax.map(final_body, after_row).reshape(NUM_SEQ, RESIDUES, MSA_CH)
```

```python
import functools

import jax
import jax.numpy as jnp
from jax import lax
from jax.experimental import pallas as pl
from jax.experimental.pallas import tpu as pltpu
from jax.sharding import PartitionSpec as P

LN_EPS = 1.0e-5
MASK_BIG = 1.0e9
MEAN_EPS = 1.0e-10
LOG2E = 1.4426950408889634

N_DEV = 4
N_LOC = 8
N_SEQ = 32
N_RES = 384
BLK = 96
N_CH = 256
N_PAIR = 128
N_HEADS = 8
HEAD_DIM = 32
SCALE = HEAD_DIM ** -0.5
Z_ROWS = 8
Z_CHUNKS = BLK // Z_ROWS
COL_BLK = 16
F32 = jnp.float32
BF16 = jnp.bfloat16
MESH = pl.DeviceIdType.MESH


def dot(a, b):
    return jnp.dot(a, b, preferred_element_type=F32)


def dot_nt(a, b):
    return lax.dot_general(a, b, (((1,), (1,)), ((), ())), preferred_element_type=F32)


def sigmoid(x):
    return 0.5 * jnp.tanh(0.5 * x) + 0.5


def layer_norm(x):
    x = x.astype(F32)
    centered = x - jnp.mean(x, axis=-1, keepdims=True)
    var = jnp.mean(centered * centered, axis=-1, keepdims=True)
    return (centered * lax.rsqrt(var + LN_EPS)).astype(BF16)


def row_kernel(e_ref, mask_ref, z_ref, w_pair_ref, w_in_ref, w_out_ref, e1_ref, mask_all_ref,
               z_buf, proj, bias_all, bias_tmp, bias_f32, q_heads, probs, gated, e1_send,
               z_sem, b_send, b_recv, r_send, r_recv, o_send, o_recv, m_send, m_recv, m_loc):
    me = lax.axis_index("seq")
    x, c = me // 2, me % 2
    peer = x * 2 + (1 - c)
    cross = (1 - x) * 2 + c
    diag = (1 - x) * 2 + (1 - c)

    barrier = pltpu.get_barrier_semaphore()
    for other in (peer, cross, diag):
        pl.semaphore_signal(barrier, inc=1, device_id={"seq": other}, device_id_type=MESH)

    def z_copy(i):
        return pltpu.make_async_copy(z_ref.at[pl.ds(i * Z_ROWS * N_RES, Z_ROWS * N_RES)], z_buf.at[i], z_sem.at[i])

    for i in range(Z_CHUNKS):
        z_copy(i).start()
    pl.semaphore_wait(barrier, 3)

    def mask_copy(k, other):
        return pltpu.make_async_remote_copy(
            src_ref=mask_ref, dst_ref=mask_all_ref.at[pl.ds(pl.multiple_of(me * N_LOC, N_LOC), N_LOC)],
            send_sem=m_send.at[k], recv_sem=m_recv.at[k], device_id={"seq": other}, device_id_type=MESH)

    mask_copies = [mask_copy(k, other) for k, other in enumerate((peer, cross, diag))]
    for copy in mask_copies:
        copy.start()
    mask_own = pltpu.make_async_copy(mask_ref, mask_all_ref.at[pl.ds(pl.multiple_of(me * N_LOC, N_LOC), N_LOC)], m_loc)
    mask_own.start()

    eye = (lax.broadcasted_iota(jnp.int32, (N_HEADS, N_HEADS), 0) == lax.broadcasted_iota(jnp.int32, (N_HEADS, N_HEADS), 1)).astype(BF16)
    w_pair_t = dot_nt(eye, w_pair_ref[...]).astype(BF16)
    rows = Z_ROWS * N_HEADS

    def bias_copy(k, other, i):
        part = bias_all.at[me, pl.ds(pl.multiple_of(i * rows, rows), rows)]
        return pltpu.make_async_remote_copy(
            src_ref=part, dst_ref=part, send_sem=b_send.at[k, i], recv_sem=b_recv.at[k, i],
            device_id={"seq": other}, device_id_type=MESH)

    def bias_chunk(i, carry):
        z_copy(i).wait()
        z_t = z_buf[i].T.astype(F32)
        centered = z_t - jnp.mean(z_t, axis=0, keepdims=True)
        var = jnp.mean(centered * centered, axis=0, keepdims=True)
        normed = (centered * lax.rsqrt(var + LN_EPS)).astype(BF16)
        out = dot(w_pair_t, normed)
        parts = [out[:, r * N_RES:(r + 1) * N_RES] for r in range(Z_ROWS)]
        bias_all[me, pl.ds(pl.multiple_of(i * rows, rows), rows)] = jnp.concatenate(parts, axis=0).astype(BF16)
        bias_copy(0, cross, i).start()
        bias_copy(1, peer, i).start()
        return carry

    lax.fori_loop(0, Z_CHUNKS, bias_chunk, 0)

    def project(s, carry):
        proj[s] = dot(layer_norm(e_ref[s]), w_in_ref[...]).astype(BF16)
        return carry

    lax.fori_loop(0, N_LOC, project, 0)

    def relay_copy(owner):
        return pltpu.make_async_remote_copy(
            src_ref=bias_all.at[owner], dst_ref=bias_all.at[owner], send_sem=r_send, recv_sem=r_recv,
            device_id={"seq": peer}, device_id_type=MESH)

    def out_copy(k, owner):
        return pltpu.make_async_remote_copy(
            src_ref=e1_send.at[k], dst_ref=e1_ref.at[pl.ds(pl.multiple_of(me * N_LOC, N_LOC), N_LOC)],
            send_sem=o_send.at[k], recv_sem=o_recv.at[k], device_id={"seq": owner}, device_id_type=MESH)

    def out_own():
        return pltpu.make_async_copy(e1_send.at[0], e1_ref.at[pl.ds(pl.multiple_of(me * N_LOC, N_LOC), N_LOC)], o_send.at[0])

    lane_head = lax.broadcasted_iota(jnp.int32, (1, N_CH), 1) // HEAD_DIM

    def block(k, carry):
        dx, dc = ((k + 1) // 2) % 2, k // 2
        owner = ((x + dx) % 2) * 2 + (c + dc) % 2

        @pl.when(k == 1)
        def _():
            def wait_chunk(i, inner):
                bias_copy(0, cross, i).wait_recv()
                return inner
            lax.fori_loop(0, Z_CHUNKS, wait_chunk, 0)
            relay_copy(cross).start()

        @pl.when(k == 2)
        def _():
            relay_copy(diag).wait_recv()

        @pl.when(k == 3)
        def _():
            def wait_chunk(i, inner):
                bias_copy(1, peer, i).wait_recv()
                return inner
            lax.fori_loop(0, Z_CHUNKS, wait_chunk, 0)

        for t in range(N_RES // 128):
            bias_tmp[t] = bias_all[owner, :, t * 128:(t + 1) * 128].astype(F32) * LOG2E
        for t in range(N_RES // 128):
            for h in range(N_HEADS):
                bias_f32[pl.ds(h * BLK, BLK), t * 128:(t + 1) * 128] = bias_tmp[t, pl.ds(h, BLK, stride=N_HEADS), :]

        start = pl.multiple_of(owner * BLK, BLK)

        def one_seq(s, inner):
            q = proj[s, pl.ds(start, BLK), 0:N_CH]
            for h in range(N_HEADS):
                q_heads[pl.ds(h * BLK, BLK)] = jnp.where(lane_head == h, q, jnp.zeros_like(q))
            logits = dot_nt(q_heads[...], proj[s, :, N_CH:2 * N_CH])
            mask_bias = (MASK_BIG * LOG2E) * (mask_ref[pl.ds(s, 1)].astype(F32) - 1.0)
            logits = logits * (SCALE * LOG2E) + bias_f32[...] + mask_bias
            top = jnp.max(logits, axis=-1, keepdims=True)
            weights = jnp.exp2(logits - top)
            total = jnp.sum(weights, axis=-1, keepdims=True)
            probs[...] = (weights * (1.0 / total)).astype(BF16)
            full = dot(probs[...], proj[s, :, 2 * N_CH:3 * N_CH])
            att = full[0:BLK]
            for h in range(1, N_HEADS):
                att = jnp.where(lane_head == h, full[h * BLK:(h + 1) * BLK], att)
            gate = sigmoid(proj[s, pl.ds(start, BLK), 3 * N_CH:4 * N_CH].astype(F32))
            gated[pl.ds(pl.multiple_of(s * BLK, BLK), BLK)] = (gate * att).astype(BF16)
            return inner

        lax.fori_loop(0, N_LOC, one_seq, 0)
        update = dot(gated[...], w_out_ref[...])
        act = e_ref[:, pl.ds(start, BLK), :].astype(F32).reshape(N_LOC * BLK, N_CH)
        e1_send[k] = (act + update).astype(BF16).reshape(N_LOC, BLK, N_CH)

        @pl.when(k == 0)
        def _():
            out_own().start()

        @pl.when(k > 0)
        def _():
            out_copy(k, owner).start()

        return carry

    lax.fori_loop(0, N_DEV, block, 0)

    out_own().wait()
    for k, owner in ((1, cross), (2, diag), (3, peer)):
        out_copy(k, owner).wait()
    for copy in mask_copies:
        copy.wait()
    mask_own.wait()
    relay_copy(cross).wait_send()

    def wait_sent(i, carry):
        bias_copy(0, cross, i).wait_send()
        bias_copy(1, peer, i).wait_send()
        return carry

    lax.fori_loop(0, Z_CHUNKS, wait_sent, 0)


def row_stage(msa_act, msa_mask, pair_act, w_pair_bias, w_row_in, w_row_out):
    vmem = pl.BlockSpec(memory_space=pltpu.VMEM)
    hbm = pl.BlockSpec(memory_space=pl.ANY)
    dma = pltpu.SemaphoreType.DMA
    return pl.pallas_call(
        row_kernel,
        out_shape=(jax.ShapeDtypeStruct((N_SEQ, BLK, N_CH), BF16), jax.ShapeDtypeStruct((N_SEQ, N_RES), jnp.int32)),
        in_specs=[vmem, vmem, hbm, vmem, vmem, vmem],
        out_specs=(hbm, hbm),
        scratch_shapes=[
            pltpu.VMEM((Z_CHUNKS, Z_ROWS * N_RES, N_PAIR), BF16),
            pltpu.VMEM((N_LOC, N_RES, 4 * N_CH), BF16),
            pltpu.VMEM((N_DEV, BLK * N_HEADS, N_RES), BF16),
            pltpu.VMEM((N_RES // 128, BLK * N_HEADS, 128), F32),
            pltpu.VMEM((BLK * N_HEADS, N_RES), F32),
            pltpu.VMEM((BLK * N_HEADS, N_CH), BF16),
            pltpu.VMEM((BLK * N_HEADS, N_RES), BF16),
            pltpu.VMEM((N_LOC * BLK, N_CH), BF16),
            pltpu.VMEM((N_DEV, N_LOC, BLK, N_CH), BF16),
            dma((Z_CHUNKS,)),
            dma((2, Z_CHUNKS)), dma((2, Z_CHUNKS)),
            dma, dma,
            dma((N_DEV,)), dma((N_DEV,)),
            dma((3,)), dma((3,)), dma,
        ],
        compiler_params=pltpu.CompilerParams(collective_id=0, has_side_effects=True, vmem_limit_bytes=60 * 2 ** 20),
        name="row_stage",
    )(msa_act, msa_mask, pair_act, w_pair_bias, w_row_in, w_row_out)


def col_kernel(e1_ref, mask_ref, w_in_ref, w_out_ref, w_t1_ref, w_t2_ref, out_ref, w_big):
    step = pl.program_id(0)
    me = lax.axis_index("seq")
    n_rows = N_SEQ * COL_BLK

    @pl.when(step == 0)
    def _():
        n_in = w_in_ref.shape[1]
        r = lax.broadcasted_iota(jnp.int32, (n_in, 4 * N_CH), 0)
        col = lax.broadcasted_iota(jnp.int32, (n_in, 4 * N_CH), 1)
        part = col // N_CH
        src = jnp.where(part == 0, col, jnp.where(part == 3, col - 3 * N_CH + N_CH + 2 * HEAD_DIM,
                                                  N_CH + (part - 1) * HEAD_DIM + col % HEAD_DIM))
        w_big[...] = dot(w_in_ref[...], (r == src).astype(BF16)).astype(BF16)

    x = e1_ref[...].reshape(n_rows, N_CH)
    proj = dot(layer_norm(x), w_big[...]).astype(BF16)
    first = me * BLK + step * COL_BLK
    lane = lax.broadcasted_iota(jnp.int32, (N_SEQ, COL_BLK, N_RES), 2)
    res = lax.broadcasted_iota(jnp.int32, (N_SEQ, COL_BLK, N_RES), 1)
    picked = jnp.where(lane == first + res, mask_ref[...].astype(F32)[:, None, :], 0.0).astype(BF16).reshape(n_rows, N_RES)
    mask = dot(picked, jnp.ones((N_RES, N_CH), BF16)).reshape(N_SEQ, COL_BLK, N_CH)

    q = proj[:, 0:N_CH].astype(F32).reshape(N_SEQ, COL_BLK, N_CH)
    k = proj[:, N_CH:2 * N_CH].astype(F32).reshape(N_SEQ, COL_BLK, N_CH)
    v = proj[:, 2 * N_CH:3 * N_CH].astype(F32).reshape(N_SEQ, COL_BLK, N_CH)
    g = proj[:, 3 * N_CH:4 * N_CH].astype(F32).reshape(N_SEQ, COL_BLK, N_CH)
    q_mean = (jnp.sum(mask * q, axis=0) / (jnp.sum(mask, axis=0) + MEAN_EPS)).astype(BF16).astype(F32)
    prod = (q_mean[None] * k).reshape(n_rows, N_CH)
    high = prod.astype(BF16)
    low = (prod - high.astype(F32)).astype(BF16)
    same_head = (lax.broadcasted_iota(jnp.int32, (N_CH, N_CH), 0) // HEAD_DIM == lax.broadcasted_iota(jnp.int32, (N_CH, N_CH), 1) // HEAD_DIM).astype(BF16)
    logits = (dot(high, same_head) + dot(low, same_head)).reshape(N_SEQ, COL_BLK, N_CH)
    logits = logits * (SCALE * LOG2E) + (MASK_BIG * LOG2E) * (mask - 1.0)
    weights = jnp.exp2(logits - jnp.max(logits, axis=0)[None])
    o = jnp.sum(weights * v, axis=0) / jnp.sum(weights, axis=0)
    gated = (sigmoid(g) * o[None]).astype(BF16).reshape(n_rows, N_CH)
    e2 = (x.astype(F32) + dot(gated, w_out_ref[...])).astype(BF16)
    hidden = jnp.maximum(dot(layer_norm(e2), w_t1_ref[...]), 0.0).astype(BF16)
    e3 = (e2.astype(F32) + dot(hidden, w_t2_ref[...])).astype(BF16)
    out_ref[...] = e3.reshape(N_SEQ, COL_BLK, N_CH)


def col_stage(e1, mask_all, w_col_in, w_col_out, w_trans_in, w_trans_out):
    whole = lambda a: pl.BlockSpec(a.shape, lambda i: (0, 0))
    blk = pl.BlockSpec((N_SEQ, COL_BLK, N_CH), lambda i: (0, i, 0))
    return pl.pallas_call(
        col_kernel,
        grid=(BLK // COL_BLK,),
        out_shape=jax.ShapeDtypeStruct((N_SEQ, BLK, N_CH), BF16),
        in_specs=[blk, whole(mask_all), whole(w_col_in), whole(w_col_out), whole(w_trans_in), whole(w_trans_out)],
        out_specs=blk,
        scratch_shapes=[pltpu.VMEM((N_CH, 4 * N_CH), BF16)],
        compiler_params=pltpu.CompilerParams(dimension_semantics=("arbitrary",), vmem_limit_bytes=60 * 2 ** 20),
        name="col_stage",
    )(e1, mask_all, w_col_in, w_col_out, w_trans_in, w_trans_out)


def solution(mesh):
    def local_block(msa_act, msa_mask, pair_act, w_pair_bias, w_row_in, w_row_out, w_col_in, w_col_out, w_trans_in, w_trans_out):
        pairs = pair_act.reshape(BLK * N_RES, N_PAIR)
        e1, mask_all = row_stage(msa_act, msa_mask, pairs, w_pair_bias, w_row_in, w_row_out)
        return col_stage(e1, mask_all, w_col_in, w_col_out, w_trans_in, w_trans_out)

    rows_spec = P(('batch', 'seq'))
    return jax.shard_map(local_block, mesh=mesh, in_specs=(rows_spec, rows_spec, rows_spec, P(), P(), P(), P(), P(), P(), P()), out_specs=P('batch', 'seq'), check_vma=False)
```
